8 devices in a mesh: rep: 2 (over y, z), dp: 4 (over x, core).
Axes of the slice: x: 2, y: 2, z: 1, core: 2. Of those that a mesh axis runs over, the one named last changes fastest.
Arguments:
- g_w_gate: bfloat16 [8, 2, 1024, 2816], P(('rep', 'dp')), parts along dimension 0
- g_w_up: bfloat16 [8, 2, 1024, 2816], P(('rep', 'dp')), parts along dimension 0
- g_w_down: bfloat16 [8, 2, 2816, 1024], P(('rep', 'dp')), parts along dimension 0
- w_gate: bfloat16 [2, 1024, 2816], replicated
- w_up: bfloat16 [2, 1024, 2816], replicated
- w_down: bfloat16 [2, 2816, 1024], replicated
- m_w_gate: float32 [2, 1024, 2816], P(None, 'dp')
- m_w_up: float32 [2, 1024, 2816], P(None, 'dp')
- m_w_down: float32 [2, 2816, 1024], P(None, 'dp')
- v_w_gate: float32 [2, 1024, 2816], P(None, 'dp')
- v_w_up: float32 [2, 1024, 2816], P(None, 'dp')
- v_w_down: float32 [2, 2816, 1024], P(None, 'dp')
Outputs:
- output 1: bfloat16 [4, 1024, 2816], P('rep'), parts along dimension 0
- output 2: bfloat16 [4, 1024, 2816], P('rep'), parts along dimension 0
- output 3: bfloat16 [4, 2816, 1024], P('rep'), parts along dimension 0
- output 4: float32 [4, 1024, 2816], P('rep', 'dp'), parts along dimension 0
- output 5: float32 [4, 1024, 2816], P('rep', 'dp'), parts along dimension 0
- output 6: float32 [4, 2816, 1024], P('rep', 'dp'), parts along dimension 0
- output 7: float32 [4, 1024, 2816], P('rep', 'dp'), parts along dimension 0
- output 8: float32 [4, 1024, 2816], P('rep', 'dp'), parts along dimension 0
- output 9: float32 [4, 2816, 1024], P('rep', 'dp'), parts along dimension 0
There are 2 independent parts. The reference program is written for one: setup_inputs(seed, part) draws one part's arguments, and reference() takes and returns one part's arrays. A program takes and returns all parts, laid end to end along the dimension named above; an argument that names none is the same for every part.
All inputs are finite; a program needn't handle non-finite values.
Results may differ from the reference program's by a relative error of at most 0.022.
Values are sent between devices in bfloat16 or wider.
A program may use at most 2 GiB of HBM per device.

```python
import jax
import jax.numpy as jnp
from jax import lax

DEVICES = 4
D = 1024
FF = 2816
LAYERS = 2
NAMES = ("w_gate", "w_up", "w_down")
SHAPES = {"w_gate": (LAYERS, D, FF), "w_up": (LAYERS, D, FF), "w_down": (LAYERS, FF, D)}


def setup_inputs(seed: int = 0, part: int = 0) -> dict:
    kz, *keys = jax.random.split(jax.random.key(seed), 1 + 5 * len(NAMES))
    loud = 2.0 ** jax.random.uniform(kz, (), jnp.float32, -1.0, 1.0)
    drawn = {}
    for name, key, both in zip(NAMES, keys[:3], keys[3:6], strict=True):
        own = jax.random.normal(jax.random.fold_in(key, part), (DEVICES, *SHAPES[name]), jnp.float32)
        shared = jax.random.normal(jax.random.fold_in(both, part), SHAPES[name], jnp.float32)
        drawn["g_" + name] = (loud * (0.7 * shared / DEVICES + 0.7 * own * DEVICES**-0.5)).astype(jnp.bfloat16)
    for name, key in zip(NAMES, keys[6:9], strict=True):
        drawn[name] = (jax.random.normal(key, SHAPES[name], jnp.float32) * SHAPES[name][1] ** -0.5).astype(jnp.bfloat16)
    for name, key in zip(NAMES, keys[9:12], strict=True):
        drawn["m_" + name] = loud * 0.5 * jax.random.normal(key, SHAPES[name], jnp.float32)
    for name, key in zip(NAMES, keys[12:15], strict=True):
        drawn["v_" + name] = loud * loud * jax.random.uniform(key, SHAPES[name], jnp.float32, 0.5, 1.5)
    return drawn


def adamw(w, m, v, g):
    m = 0.9 * m + 0.1 * g
    v = 0.95 * v + 0.05 * g * g
    step = m * lax.rsqrt(v + 1e-8) + 0.1 * w
    return (w - 0.02 * step).astype(jnp.bfloat16), m, v


def reference(g_w_gate, g_w_up, g_w_down, w_gate, w_up, w_down, m_w_gate, m_w_up, m_w_down, v_w_gate, v_w_up, v_w_down):
    def total(terms):
        return lax.scan(lambda so_far, term: (so_far + term.astype(jnp.float32), None), jnp.zeros(terms.shape[1:], jnp.float32), terms)[0]

    gradients = [total(terms).astype(jnp.bfloat16).astype(jnp.float32) for terms in (g_w_gate, g_w_up, g_w_down)]
    new = [
        adamw(w.astype(jnp.float32), m, v, g)
        for w, m, v, g in zip((w_gate, w_up, w_down), (m_w_gate, m_w_up, m_w_down), (v_w_gate, v_w_up, v_w_down), gradients, strict=True)
    ]
    return tuple(one[which] for which in range(3) for one in new)
```

```python
import functools

import jax
import jax.numpy as jnp
from jax import lax
from jax.experimental import pallas as pl
from jax.experimental.pallas import tpu as pltpu
from jax.sharding import PartitionSpec as P


LAYERS = 2
SUBS = 4
PER = LAYERS * SUBS
WEIGHTS = 3
GATHERED = 2
CHUNKS = PER * WEIGHTS
SLOTS = 3
ANY = pl.BlockSpec(memory_space=pl.ANY)
VMEM_LIMIT = 60 * 2**20
WIDTH = 256


def add_into(dst, at, own, rows, cols):
    def body(i, _):
        r = pl.ds(pl.multiple_of(i * 16, 16), 16)
        for c in range(0, cols, WIDTH):
            s = pl.ds(c, WIDTH)
            dst[(*at, r, s)] = (dst[(*at, r, s)].astype(jnp.float32) + own[r, s].astype(jnp.float32)).astype(jnp.bfloat16)
        return 0

    lax.fori_loop(0, rows // 16, body, 0)


def step_into(x, at, mine, pair, pair_at, w, m, v, rows, cols):
    def body(i, _):
        r = pl.ds(pl.multiple_of(i * 16, 16), 16)
        for c in range(0, cols, WIDTH):
            s = pl.ds(c, WIDTH)
            g = mine[r, s].astype(jnp.float32) + pair[(*pair_at, r, s)].astype(jnp.float32) + x[(*at, r, s)].astype(jnp.float32)
            g = g.astype(jnp.bfloat16).astype(jnp.float32)
            nm = 0.9 * m[r, s] + 0.1 * g
            nv = 0.95 * v[r, s] + 0.05 * g * g
            old = w[r, s].astype(jnp.float32)
            step = nm * lax.rsqrt(nv + 1e-8) + 0.1 * old
            x[(*at, r, s)] = (old - 0.02 * step).astype(jnp.bfloat16)
            m[r, s] = nm
            v[r, s] = nv
        return 0

    lax.fori_loop(0, rows // 16, body, 0)


def main_kernel(dims, *refs):
    g, w, m, v = (refs[i : i + 3] for i in (0, 3, 6, 9))
    wf, mo, vo = (refs[12 + i : 15 + i] for i in (0, 3, 6))
    pieces = refs[21:25]
    (rv_a, rv_b, xr_a, xr_b, ob_a, ob_b, oc_a, oc_b, wc_a, wc_b, mc_a, mc_b, vc_a, vc_b,
     d_s, d_r, x_s, x_r, ax_s, ax_r, o_s, o_r, f_s, f_r, lb, lc, st) = refs[25:]
    me = lax.axis_index("dp")
    x, k = me // 2, me % 2
    xo, ko = 1 - x, 1 - k
    partner, across = {"dp": 2 * x + ko}, {"dp": 2 * xo + k}

    barrier = pltpu.get_barrier_semaphore()
    for d in (partner, across):
        pl.semaphore_signal(barrier, inc=1, device_id=d, device_id_type=pl.DeviceIdType.MESH)
    pl.semaphore_wait(barrier, 2)

    def remote(src, dst, s, r, to):
        return pltpu.make_async_remote_copy(src_ref=src, dst_ref=dst, send_sem=s, recv_sem=r, device_id=to, device_id_type=pl.DeviceIdType.MESH)

    class Chunk:
        def __init__(self, c):
            self.c, self.i = c, c // PER
            j = c % PER
            self.l, self.sub = j // SUBS, j % SUBS
            a = self.i < 2
            self.slot = c if a else j
            self.rows, self.cols = dims[self.i][0] // SUBS, dims[self.i][1]
            self.r = pl.ds(self.sub * self.rows, self.rows)
            self.rv, self.xr = (rv_a, xr_a) if a else (rv_b, xr_b)
            self.ob = (ob_a if a else ob_b).at[c % 2]
            p = c % SLOTS
            self.oc, self.wc, self.mc, self.vc = (t.at[p] for t in ((oc_a, wc_a, mc_a, vc_a) if a else (oc_b, wc_b, mc_b, vc_b)))
            self.whole = wf[self.i].at[self.l, x, k, self.r]
            self.pair = remote(g[self.i].at[self.l, :, ko, self.r], self.rv.at[self.slot], d_s.at[c], d_r.at[c], partner)
            self.load_b = pltpu.make_async_copy(g[self.i].at[self.l, xo, k, self.r], self.ob, lb.at[c % 2])
            self.cross = remote(self.rv.at[self.slot, xo], self.xr.at[self.slot], x_s.at[c], x_r.at[c], across)
            block = (self.l, self.r)
            self.loads = [
                pltpu.make_async_copy(g[self.i].at[self.l, x, k, self.r], self.oc, lc.at[p, 0]),
                pltpu.make_async_copy(w[self.i].at[self.l, x, k, self.r], self.wc, lc.at[p, 1]),
                pltpu.make_async_copy(m[self.i].at[block], self.mc, lc.at[p, 2]),
                pltpu.make_async_copy(v[self.i].at[block], self.vc, lc.at[p, 3]),
            ]
            new = self.xr.at[self.slot]
            self.stores = [
                pltpu.make_async_copy(self.mc, mo[self.i].at[block], st.at[p, 0]),
                pltpu.make_async_copy(self.vc, vo[self.i].at[block], st.at[p, 1]),
                pltpu.make_async_copy(new, self.whole, st.at[p, 2]),
            ]
            self.own = remote(new, self.whole, o_s.at[c], o_r.at[c], partner)
            if self.i < GATHERED:
                far = wf[self.i].at[self.l, xo, k, self.r]
                self.gather = remote(new, self.whole, ax_s.at[c], ax_r.at[c], across)
                self.forward = remote(far, far, f_s.at[c], f_r.at[c], partner)
            else:
                piece = pieces[j // 2]
                self.stores.append(pltpu.make_async_copy(new, piece.at[pl.ds((j % 2) * self.rows, self.rows)], st.at[p, 3]))

    chunks = [Chunk(c) for c in range(CHUNKS)]
    for ch in chunks:
        ch.pair.start()
    for ch in chunks[:2]:
        ch.load_b.start()
    for ch in chunks:
        ch.load_b.wait()
        ch.pair.wait_recv()
        add_into(ch.rv, (ch.slot, xo), ch.ob, ch.rows, ch.cols)
        ch.cross.start()
        if ch.c + 2 < CHUNKS:
            chunks[ch.c + 2].load_b.start()
    for ch in chunks[:2]:
        for one in ch.loads:
            one.start()
    for ch in chunks:
        for one in ch.loads:
            one.wait()
        ch.cross.wait_recv()
        step_into(ch.xr, (ch.slot,), ch.oc, ch.rv, (ch.slot, x), ch.wc, ch.mc, ch.vc, ch.rows, ch.cols)
        if ch.i < GATHERED:
            ch.gather.start()
        ch.own.start()
        for one in ch.stores:
            one.start()
        if ch.c >= 1:
            for one in chunks[ch.c - 1].stores:
                one.wait()
        if ch.c + 2 < CHUNKS:
            for one in chunks[ch.c + 2].loads:
                one.start()
    for one in chunks[-1].stores:
        one.wait()
    for ch in chunks:
        if ch.i < GATHERED:
            ch.gather.wait_recv()
            ch.forward.start()
    for ch in chunks:
        ch.pair.wait_send()
        ch.cross.wait_send()
        ch.own.wait()
        if ch.i < GATHERED:
            ch.gather.wait_send()
            ch.forward.wait()


def communicate(g, w, m, v):
    dims = [one.shape[3:] for one in g]
    (ra, ca), (rb, cb) = dims[0], dims[2]
    ra, rb = ra // SUBS, rb // SUBS
    sd = jax.ShapeDtypeStruct
    bf, f32 = jnp.bfloat16, jnp.float32
    dma = pltpu.SemaphoreType.DMA
    out = (
        *(sd(one.shape, bf) for one in w),
        *(sd(one.shape, f32) for one in m),
        *(sd(one.shape, f32) for one in v),
        *(sd((2 * rb, cb), bf) for _ in range(PER // 2)),
    )
    scratch = [
        pltpu.VMEM((2 * PER, 2, ra, ca), bf), pltpu.VMEM((PER, 2, rb, cb), bf),
        pltpu.VMEM((2 * PER, ra, ca), bf), pltpu.VMEM((PER, rb, cb), bf),
        pltpu.VMEM((2, ra, ca), bf), pltpu.VMEM((2, rb, cb), bf),
        pltpu.VMEM((SLOTS, ra, ca), bf), pltpu.VMEM((SLOTS, rb, cb), bf),
        pltpu.VMEM((SLOTS, ra, ca), bf), pltpu.VMEM((SLOTS, rb, cb), bf),
        pltpu.VMEM((SLOTS, ra, ca), f32), pltpu.VMEM((SLOTS, rb, cb), f32),
        pltpu.VMEM((SLOTS, ra, ca), f32), pltpu.VMEM((SLOTS, rb, cb), f32),
        *(dma((CHUNKS,)) for _ in range(4)),
        *(dma((GATHERED * PER,)) for _ in range(2)),
        *(dma((CHUNKS,)) for _ in range(2)),
        *(dma((GATHERED * PER,)) for _ in range(2)),
        dma((2,)), dma((SLOTS, 4)), dma((SLOTS, 4)),
    ]
    return pl.pallas_call(
        functools.partial(main_kernel, dims),
        out_shape=out,
        in_specs=[ANY] * 12,
        out_specs=[ANY] * len(out),
        scratch_shapes=scratch,
        compiler_params=pltpu.CompilerParams(collective_id=0, has_side_effects=True, vmem_limit_bytes=VMEM_LIMIT),
        name="communicate",
    )(*g, *w, *m, *v)


def copy_kernel(n, _, *refs):
    for src, dst in zip(refs[:n], refs[n:], strict=True):
        dst[...] = src[...]


def copy_out(x, wf, mo, vo):
    specs = []
    for one in wf[:2]:
        rows, cols = one.shape[3:]
        specs.append(pl.BlockSpec((1, 1, 1, rows, cols), lambda i, _: (i // 4, i // 2 % 2, i % 2, 0, 0)))
    rows, cols = wf[2].shape[3:]
    specs.append(pl.BlockSpec((1, 1, 1, rows // 2, cols), lambda i, s: (i // 4, s[0], i // 2 % 2, i % 2, 0)))
    for one in (*mo, *vo):
        _, rows, cols = one.shape
        specs.append(pl.BlockSpec((1, rows // SUBS, cols), lambda i, _: (i // SUBS, i % SUBS, 0)))
    arrays = (*wf, *mo, *vo)
    size = sum(2 * one.size * one.dtype.itemsize for one in arrays)
    return pl.pallas_call(
        functools.partial(copy_kernel, len(arrays)),
        out_shape=[jax.ShapeDtypeStruct(one.shape, one.dtype) for one in arrays],
        grid_spec=pltpu.PrefetchScalarGridSpec(num_scalar_prefetch=1, grid=(PER,), in_specs=specs, out_specs=specs),
        cost_estimate=pl.CostEstimate(flops=0, bytes_accessed=size, transcendentals=0),
        compiler_params=pltpu.CompilerParams(vmem_limit_bytes=VMEM_LIMIT),
        name="copy_out",
    )(x.reshape(1), *arrays)


def place_kernel(l, half, rows, cross, far, whole, out, buf, ld, st):
    me = lax.axis_index("dp")
    x, k = me // 2, me % 2
    r = pl.ds(half * rows, rows)
    loads = [pltpu.make_async_copy(cross, buf.at[0], ld.at[0]), pltpu.make_async_copy(far, buf.at[1], ld.at[1])]
    stores = [
        pltpu.make_async_copy(buf.at[0], out.at[l, 1 - x, k, r], st.at[0]),
        pltpu.make_async_copy(buf.at[1], out.at[l, 1 - x, 1 - k, r], st.at[1]),
    ]
    for one in loads:
        one.start()
    for a, b in zip(loads, stores, strict=True):
        a.wait()
        b.start()
    for one in stores:
        one.wait()


def place(l, half, cross, far, whole):
    rows, cols = cross.shape
    return pl.pallas_call(
        functools.partial(place_kernel, l, half, rows),
        out_shape=jax.ShapeDtypeStruct(whole.shape, whole.dtype),
        in_specs=[ANY] * 3,
        out_specs=ANY,
        scratch_shapes=[pltpu.VMEM((2, rows, cols), whole.dtype), pltpu.SemaphoreType.DMA((2,)), pltpu.SemaphoreType.DMA((2,))],
        input_output_aliases={2: 0},
        cost_estimate=pl.CostEstimate(flops=0, bytes_accessed=8 * cross.size, transcendentals=0),
        name=f"place_{l}_{half}",
    )(cross, far, whole)


def solution(mesh):
    swap_x, swap_core = [(i, (i + 2) % 4) for i in range(4)], [(i, i ^ 1) for i in range(4)]

    def step(*arrays):
        terms, weights, m, v = (arrays[i : i + 3] for i in (0, 3, 6, 9))

        def cut(a):
            return a.reshape(LAYERS, 2, 2, a.shape[-2] // 4, a.shape[-1])

        done = communicate([cut(t) for t in terms], [cut(w) for w in weights], m, v)
        wf, mo, vo, pieces = done[:3], done[3:6], done[6:9], done[9:]
        cross = [lax.ppermute(p, "dp", swap_x) for p in pieces]
        x = (lax.axis_index("dp") // 2).astype(jnp.int32)
        copied = copy_out(x, wf, mo, vo)
        down, far = copied[2], []
        for i, p in enumerate(cross):
            cross[i], down = lax.optimization_barrier((p, down))
            far.append(lax.ppermute(cross[i], "dp", swap_core))
        for i, (a, b) in enumerate(zip(cross, far, strict=True)):
            down = place(i // 2, i % 2, a, b, down)
        whole = [a.reshape(w.shape) for a, w in zip((*copied[:2], down), weights, strict=True)]
        return (*whole, *copied[3:])

    all_of, cut = P(None, None, None), P(None, "dp", None)
    return jax.shard_map(
        step,
        mesh=mesh,
        in_specs=(P(("rep", "dp"), None, None, None),) * 3 + (all_of,) * 3 + (cut,) * 6,
        out_specs=(P("rep", None, None),) * 3 + (P("rep", "dp", None),) * 6,
        check_vma=False,
    )
```

```python
import functools

import jax
import jax.numpy as jnp
from jax import lax
from jax.experimental import pallas as pl
from jax.experimental.pallas import tpu as pltpu
from jax.sharding import PartitionSpec as P


LAYERS = 2
SUBS = 4
PER = LAYERS * SUBS
WEIGHTS = 3
GATHERED = 2
CHUNKS = PER * WEIGHTS
SLOTS = 3
AHEAD = 4
PARTS = 4
PIECES = ((0, 1), (2, 3), (4, 5), (6,), (7,))
LATE = GATHERED * PER - 1
ANY = pl.BlockSpec(memory_space=pl.ANY)
VMEM_LIMIT = 60 * 2**20
VMEM_ALL = 67043328
WIDTH = 256


def add_into(dst, at, own, first, rows, cols):
    def body(i, _):
        r = pl.ds(pl.multiple_of(first + i * 16, 16), 16)
        for c in range(0, cols, WIDTH):
            s = pl.ds(c, WIDTH)
            dst[(*at, r, s)] = (dst[(*at, r, s)].astype(jnp.float32) + own[r, s].astype(jnp.float32)).astype(jnp.bfloat16)
        return 0

    lax.fori_loop(0, rows // 16, body, 0)


def step_into(x, at, mine, pair, pair_at, w, m, v, rows, cols):
    def body(i, _):
        r = pl.ds(pl.multiple_of(i * 16, 16), 16)
        for c in range(0, cols, WIDTH):
            s = pl.ds(c, WIDTH)
            g = mine[r, s].astype(jnp.float32) + pair[(*pair_at, r, s)].astype(jnp.float32) + x[(*at, r, s)].astype(jnp.float32)
            g = g.astype(jnp.bfloat16).astype(jnp.float32)
            nm = 0.9 * m[r, s] + 0.1 * g
            nv = 0.95 * v[r, s] + 0.05 * g * g
            old = w[r, s].astype(jnp.float32)
            step = nm * lax.rsqrt(nv + 1e-8) + 0.1 * old
            x[(*at, r, s)] = (old - 0.02 * step).astype(jnp.bfloat16)
            m[r, s] = nm
            v[r, s] = nv
        return 0

    lax.fori_loop(0, rows // 16, body, 0)


def main_kernel(dims, *refs):
    g, w, m, v = (refs[i : i + 3] for i in (0, 3, 6, 9))
    wf, mo, vo = (refs[12 + i : 15 + i] for i in (0, 3, 6))
    pieces, late = refs[21 : 21 + len(PIECES)], refs[21 + len(PIECES)]
    (rv_a, rv_b, xr_a, xr_b, first, ob_a, ob_b, oc_a, oc_b, wc_a, wc_b, mc_a, mc_b, vc_a, vc_b,
     e_s, e_r, x_s, x_r, d_s, d_r, ax_s, ax_r, o_s, o_r, f_s, f_r, lf, lb, lc, st) = refs[22 + len(PIECES) :]
    me = lax.axis_index("dp")
    x, k = me // 2, me % 2
    xo, ko = 1 - x, 1 - k
    partner, across = {"dp": 2 * x + ko}, {"dp": 2 * xo + k}

    def remote(src, dst, s, r, to):
        return pltpu.make_async_remote_copy(src_ref=src, dst_ref=dst, send_sem=s, recv_sem=r, device_id=to, device_id_type=pl.DeviceIdType.MESH)

    class Chunk:
        def __init__(self, c):
            self.c, self.i = c, c // PER
            j = c % PER
            l, sub = j // SUBS, j % SUBS
            a = self.i < 2
            self.slot = slot = c if a else j
            self.rows, self.cols = rows, _ = dims[self.i][0] // SUBS, dims[self.i][1]
            r = pl.ds(sub * rows, rows)
            self.rv, self.xr = (rv_a, xr_a) if a else (rv_b, xr_b)
            self.ob = (ob_a if a else ob_b).at[c % 2]
            p = c % SLOTS
            self.oc, self.wc, self.mc, self.vc = (t.at[p] for t in ((oc_a, wc_a, mc_a, vc_a) if a else (oc_b, wc_b, mc_b, vc_b)))
            gi, wi = g[self.i], wf[self.i]
            n = PARTS if c == 0 else 1
            self.parts = []
            for q in range(n):
                at, size, sem = q * rows // n, rows // n, q if c == 0 else c + PARTS - 1
                src = first.at[pl.ds(at, size)] if c == 0 else gi.at[l, xo, ko, r]
                sums = self.rv.at[slot, xo, pl.ds(at, size)]
                sums_there = self.rv.at[slot, xo, pl.ds(at, size)]
                pair = remote(src, sums_there, e_s.at[sem], e_r.at[sem], partner)
                cross = remote(sums, self.xr.at[slot, pl.ds(at, size)], x_s.at[sem], x_r.at[sem], across)
                self.parts.append((at, size, pair, cross))
            if c == 0:
                self.load_first = pltpu.make_async_copy(gi.at[l, xo, ko, r], first, lf)
            self.pair = remote(gi.at[l, x, ko, r], self.rv.at[slot, x], d_s.at[c], d_r.at[c], partner)
            self.load_b = pltpu.make_async_copy(gi.at[l, xo, k, r], self.ob, lb.at[c % 2])
            block = (l, r)
            self.loads = [
                pltpu.make_async_copy(gi.at[l, x, k, r], self.oc, lc.at[p, 0]),
                pltpu.make_async_copy(w[self.i].at[l, x, k, r], self.wc, lc.at[p, 1]),
                pltpu.make_async_copy(m[self.i].at[block], self.mc, lc.at[p, 2]),
                pltpu.make_async_copy(v[self.i].at[block], self.vc, lc.at[p, 3]),
            ]
            new, place = self.xr.at[slot], wi.at[l, x, k, r]
            self.stores = [
                pltpu.make_async_copy(self.mc, mo[self.i].at[block], st.at[p, 0]),
                pltpu.make_async_copy(self.vc, vo[self.i].at[block], st.at[p, 1]),
                pltpu.make_async_copy(new, place, st.at[p, 2]),
            ]
            self.own = remote(new, place, o_s.at[c], o_r.at[c], partner)
            self.gather = self.forward = None
            if self.i < GATHERED:
                far = wi.at[l, xo, k, r]
                self.gather = remote(new, late if c == LATE else place, ax_s.at[c], ax_r.at[c], across)
                if c != LATE:
                    self.forward = remote(far, far, f_s.at[c], f_r.at[c], partner)
            else:
                (q,) = (q for q, of in enumerate(PIECES) if j in of)
                self.stores.append(pltpu.make_async_copy(new, pieces[q].at[pl.ds((j - PIECES[q][0]) * rows, rows)], st.at[p, 3]))

    chunks = [Chunk(c) for c in range(CHUNKS)]
    chunks[0].load_first.start()
    for ch in chunks[:2]:
        ch.load_b.start()
        for one in ch.loads:
            one.start()

    barrier = pltpu.get_barrier_semaphore()
    for d in (partner, across):
        pl.semaphore_signal(barrier, inc=1, device_id=d, device_id_type=pl.DeviceIdType.MESH)
    pl.semaphore_wait(barrier, 2)

    chunks[0].load_first.wait()

    def send(ch):
        for _, _, pair, _ in ch.parts:
            pair.start()

    for ch in chunks[:AHEAD]:
        send(ch)
    for ch in chunks:
        ch.load_b.wait()
        for at, size, pair, cross in ch.parts:
            pair.wait_recv()
            add_into(ch.rv, (ch.slot, xo), ch.ob, at, size, ch.cols)
            cross.start()
        if ch.c + AHEAD < CHUNKS:
            send(chunks[ch.c + AHEAD])
        ch.pair.start()
        if ch.c + 2 < CHUNKS:
            chunks[ch.c + 2].load_b.start()
    for ch in chunks:
        for one in ch.loads:
            one.wait()
        ch.pair.wait_recv()
        for _, _, _, cross in ch.parts:
            cross.wait_recv()
        step_into(ch.xr, (ch.slot,), ch.oc, ch.rv, (ch.slot, x), ch.wc, ch.mc, ch.vc, ch.rows, ch.cols)
        if ch.gather:
            ch.gather.start()
        ch.own.start()
        for one in ch.stores:
            one.start()
        if ch.c >= 1:
            for one in chunks[ch.c - 1].stores:
                one.wait()
        if ch.c + 2 < CHUNKS:
            for one in chunks[ch.c + 2].loads:
                one.start()
    for one in chunks[-1].stores:
        one.wait()
    for ch in chunks:
        for _, _, pair, cross in ch.parts:
            pair.wait_send()
            cross.wait_send()
        ch.pair.wait_send()
        ch.own.wait()
    for ch in chunks:
        if ch.forward:
            ch.gather.wait_recv()
            ch.forward.start()
    for ch in chunks:
        if ch.forward:
            ch.gather.wait_send()
            ch.forward.wait()
    chunks[LATE].gather.wait()


def communicate(g, w, m, v):
    dims = [one.shape[3:] for one in g]
    (ra, ca), (rb, cb) = dims[0], dims[2]
    ra, rb = ra // SUBS, rb // SUBS
    sd = jax.ShapeDtypeStruct
    bf, f32 = jnp.bfloat16, jnp.float32
    dma = pltpu.SemaphoreType.DMA
    out = (
        *(sd(one.shape, bf) for one in w),
        *(sd(one.shape, f32) for one in m),
        *(sd(one.shape, f32) for one in v),
        *(sd((len(of) * rb, cb), bf) for of in PIECES),
        sd((ra, ca), bf),
    )
    scratch = [
        pltpu.VMEM((2 * PER, 2, ra, ca), bf), pltpu.VMEM((PER, 2, rb, cb), bf),
        pltpu.VMEM((2 * PER, ra, ca), bf), pltpu.VMEM((PER, rb, cb), bf),
        pltpu.VMEM((ra, ca), bf), pltpu.VMEM((2, ra, ca), bf), pltpu.VMEM((2, rb, cb), bf),
        pltpu.VMEM((SLOTS, ra, ca), bf), pltpu.VMEM((SLOTS, rb, cb), bf),
        pltpu.VMEM((SLOTS, ra, ca), bf), pltpu.VMEM((SLOTS, rb, cb), bf),
        pltpu.VMEM((SLOTS, ra, ca), f32), pltpu.VMEM((SLOTS, rb, cb), f32),
        pltpu.VMEM((SLOTS, ra, ca), f32), pltpu.VMEM((SLOTS, rb, cb), f32),
        *(dma((CHUNKS + PARTS - 1,)) for _ in range(4)),
        *(dma((CHUNKS,)) for _ in range(2)),
        *(dma((GATHERED * PER,)) for _ in range(2)),
        *(dma((CHUNKS,)) for _ in range(2)),
        *(dma((LATE,)) for _ in range(2)),
        dma, dma((2,)), dma((SLOTS, 4)), dma((SLOTS, 4)),
    ]
    return pl.pallas_call(
        functools.partial(main_kernel, dims),
        out_shape=out,
        in_specs=[ANY] * 12,
        out_specs=[ANY] * len(out),
        scratch_shapes=scratch,
        compiler_params=pltpu.CompilerParams(collective_id=0, has_side_effects=True, vmem_limit_bytes=VMEM_LIMIT),
        name="communicate",
    )(*g, *w, *m, *v)


def copy_kernel(n, _, *refs):
    for src, dst in zip(refs[:n], refs[n:], strict=True):
        dst[...] = src[...]


def copy_out(x, wf, mo, vo):
    specs = []
    for one in wf[:2]:
        rows, cols = one.shape[3:]
        specs.append(pl.BlockSpec((1, 1, 1, rows, cols), lambda i, _: (i // 4, i // 2 % 2, i % 2, 0, 0)))
    rows, cols = wf[2].shape[3:]
    specs.append(pl.BlockSpec((1, 1, 1, rows // 2, cols), lambda i, s: (i // 4, s[0], i // 2 % 2, i % 2, 0)))
    for one in (*mo, *vo):
        _, rows, cols = one.shape
        specs.append(pl.BlockSpec((1, rows // SUBS, cols), lambda i, _: (i // SUBS, i % SUBS, 0)))
    arrays = (*wf, *mo, *vo)
    size = sum(2 * one.size * one.dtype.itemsize for one in arrays)
    return pl.pallas_call(
        functools.partial(copy_kernel, len(arrays)),
        out_shape=[jax.ShapeDtypeStruct(one.shape, one.dtype) for one in arrays],
        grid_spec=pltpu.PrefetchScalarGridSpec(num_scalar_prefetch=1, grid=(PER,), in_specs=specs, out_specs=specs),
        cost_estimate=pl.CostEstimate(flops=0, bytes_accessed=size, transcendentals=0),
        compiler_params=pltpu.CompilerParams(vmem_limit_bytes=VMEM_ALL),
        name="copy_out",
    )(x.reshape(1), *arrays)


def place_kernel(l, first, near, far, whole, out, buf, ld, st):
    me = lax.axis_index("dp")
    x, k = me // 2, me % 2
    r = pl.ds(first, near.shape[0])
    loads = [pltpu.make_async_copy(near, buf.at[0], ld.at[0]), pltpu.make_async_copy(far, buf.at[1], ld.at[1])]
    stores = [
        pltpu.make_async_copy(buf.at[0], out.at[l, 1 - x, k, r], st.at[0]),
        pltpu.make_async_copy(buf.at[1], out.at[l, 1 - x, 1 - k, r], st.at[1]),
    ]
    for one in loads:
        one.start()
    for a, b in zip(loads, stores, strict=True):
        a.wait()
        b.start()
    for one in stores:
        one.wait()


def place(l, first, near, far, whole):
    return pl.pallas_call(
        functools.partial(place_kernel, l, first),
        out_shape=jax.ShapeDtypeStruct(whole.shape, whole.dtype),
        in_specs=[ANY] * 3,
        out_specs=ANY,
        scratch_shapes=[pltpu.VMEM((2, *near.shape), whole.dtype), pltpu.SemaphoreType.DMA((2,)), pltpu.SemaphoreType.DMA((2,))],
        input_output_aliases={2: 0},
        cost_estimate=pl.CostEstimate(flops=0, bytes_accessed=8 * near.size, transcendentals=0),
        compiler_params=pltpu.CompilerParams(vmem_limit_bytes=VMEM_ALL),
        name="place",
    )(near, far, whole)


def solution(mesh):
    swap_x, swap_core = [(i, (i + 2) % 4) for i in range(4)], [(i, i ^ 1) for i in range(4)]

    def step(*arrays):
        terms, weights, m, v = (arrays[i : i + 3] for i in (0, 3, 6, 9))

        def cut(a):
            return a.reshape(LAYERS, 2, 2, a.shape[-2] // 4, a.shape[-1])

        done = communicate([cut(t) for t in terms], [cut(w) for w in weights], m, v)
        wf, mo, vo, pieces, late = done[:3], done[3:6], done[6:9], done[9:-1], done[-1]
        cross = []
        for p in pieces:
            cross.append(lax.ppermute(p, "dp", swap_x))
        late_far = lax.ppermute(late, "dp", swap_core)
        x = (lax.axis_index("dp") // 2).astype(jnp.int32)
        gate, up, down, *moments = copy_out(x, wf, mo, vo)
        up = place(LAYERS - 1, (SUBS - 1) * late.shape[0], late, late_far, up)
        up, down = lax.optimization_barrier((up, down))
        for i, p in enumerate(cross):
            p, down = lax.optimization_barrier((p, down))
            far = lax.ppermute(p, "dp", swap_core)
            l, sub = PIECES[i][0] // SUBS, PIECES[i][0] % SUBS
            down = place(l, sub * p.shape[0] // len(PIECES[i]), p, far, down)
        whole = [a.reshape(w.shape) for a, w in zip((gate, up, down), weights, strict=True)]
        return (*whole, *moments)

    all_of, cut = P(None, None, None), P(None, "dp", None)
    return jax.shard_map(
        step,
        mesh=mesh,
        in_specs=(P(("rep", "dp"), None, None, None),) * 3 + (all_of,) * 3 + (cut,) * 6,
        out_specs=(P("rep", None, None),) * 3 + (P("rep", "dp", None),) * 6,
        check_vma=False,
    )
```

```python
import functools

import jax
import jax.numpy as jnp
from jax import lax
from jax.experimental import pallas as pl
from jax.experimental.pallas import tpu as pltpu
from jax.sharding import PartitionSpec as P


LAYERS = 2
SUBS = 4
PER = LAYERS * SUBS
WEIGHTS = 3
GATHERED = 2
CHUNKS = PER * WEIGHTS
SLOTS = 3
AHEAD = 4
PARTS = 4
PIECES = ((0, 0, 416), (0, 416, 288), (1, 0, 384), (1, 384, 208), (1, 592, 112))
LATE = GATHERED * PER - 1
ANY = pl.BlockSpec(memory_space=pl.ANY)
VMEM_LIMIT = 60 * 2**20
VMEM_ALL = 67043328
WIDTH = 256


def add_into(dst, at, own, first, rows, cols):
    def body(i, _):
        r = pl.ds(pl.multiple_of(first + i * 16, 16), 16)
        for c in range(0, cols, WIDTH):
            s = pl.ds(c, WIDTH)
            dst[(*at, r, s)] = (dst[(*at, r, s)].astype(jnp.float32) + own[r, s].astype(jnp.float32)).astype(jnp.bfloat16)
        return 0

    lax.fori_loop(0, rows // 16, body, 0)


def step_into(x, at, mine, pair, pair_at, w, m, v, rows, cols):
    def body(i, _):
        r = pl.ds(pl.multiple_of(i * 16, 16), 16)
        for c in range(0, cols, WIDTH):
            s = pl.ds(c, WIDTH)
            g = mine[r, s].astype(jnp.float32) + pair[(*pair_at, r, s)].astype(jnp.float32) + x[(*at, r, s)].astype(jnp.float32)
            g = g.astype(jnp.bfloat16).astype(jnp.float32)
            nm = 0.9 * m[r, s] + 0.1 * g
            nv = 0.95 * v[r, s] + 0.05 * g * g
            old = w[r, s].astype(jnp.float32)
            step = nm * lax.rsqrt(nv + 1e-8) + 0.1 * old
            x[(*at, r, s)] = (old - 0.02 * step).astype(jnp.bfloat16)
            m[r, s] = nm
            v[r, s] = nv
        return 0

    lax.fori_loop(0, rows // 16, body, 0)


def main_kernel(dims, *refs):
    g, w, m, v = (refs[i : i + 3] for i in (0, 3, 6, 9))
    wf, mo, vo = (refs[12 + i : 15 + i] for i in (0, 3, 6))
    pieces, late = refs[21 : 21 + len(PIECES)], refs[21 + len(PIECES)]
    (rv_a, rv_b, xr_a, xr_b, ob_a, ob_b, oc_a, oc_b, wc_a, wc_b, mc_a, mc_b, vc_a, vc_b,
     e_s, e_r, x_s, x_r, d_s, d_r, ax_s, ax_r, o_s, o_r, f_s, f_r, lb, lc, st) = refs[22 + len(PIECES) :]
    me = lax.axis_index("dp")
    x, k = me // 2, me % 2
    xo, ko = 1 - x, 1 - k
    partner, across = {"dp": 2 * x + ko}, {"dp": 2 * xo + k}

    def remote(src, dst, s, r, to):
        return pltpu.make_async_remote_copy(src_ref=src, dst_ref=dst, send_sem=s, recv_sem=r, device_id=to, device_id_type=pl.DeviceIdType.MESH)

    class Chunk:
        def __init__(self, c):
            self.c, self.i = c, c // PER
            j = c % PER
            l, sub = j // SUBS, j % SUBS
            a = self.i < 2
            self.slot = slot = c if a else j
            self.rows, self.cols = rows, _ = dims[self.i][0] // SUBS, dims[self.i][1]
            r = pl.ds(sub * rows, rows)
            self.rv, self.xr = (rv_a, xr_a) if a else (rv_b, xr_b)
            self.ob = (ob_a if a else ob_b).at[c % 2]
            p = c % SLOTS
            self.oc, self.wc, self.mc, self.vc = (t.at[p] for t in ((oc_a, wc_a, mc_a, vc_a) if a else (oc_b, wc_b, mc_b, vc_b)))
            gi, wi = g[self.i], wf[self.i]
            n = PARTS if c == 0 else 1
            self.parts = []
            for q in range(n):
                at, size, sem = q * rows // n, rows // n, q if c == 0 else c + PARTS - 1
                src = gi.at[l, xo, ko, pl.ds(sub * rows + at, size)]
                sums = self.rv.at[slot, xo, pl.ds(at, size)]
                sums_there = self.rv.at[slot, xo, pl.ds(at, size)]
                pair = remote(src, sums_there, e_s.at[sem], e_r.at[sem], partner)
                cross = remote(sums, self.xr.at[slot, pl.ds(at, size)], x_s.at[sem], x_r.at[sem], across)
                self.parts.append((at, size, pair, cross))
            self.pair = remote(gi.at[l, x, ko, r], self.rv.at[slot, x], d_s.at[c], d_r.at[c], partner)
            self.load_b = pltpu.make_async_copy(gi.at[l, xo, k, r], self.ob, lb.at[c % 2])
            block = (l, r)
            self.loads = [
                pltpu.make_async_copy(gi.at[l, x, k, r], self.oc, lc.at[p, 0]),
                pltpu.make_async_copy(w[self.i].at[l, x, k, r], self.wc, lc.at[p, 1]),
                pltpu.make_async_copy(m[self.i].at[block], self.mc, lc.at[p, 2]),
                pltpu.make_async_copy(v[self.i].at[block], self.vc, lc.at[p, 3]),
            ]
            new, place = self.xr.at[slot], wi.at[l, x, k, r]
            self.stores = [
                pltpu.make_async_copy(self.mc, mo[self.i].at[block], st.at[p, 0]),
                pltpu.make_async_copy(self.vc, vo[self.i].at[block], st.at[p, 1]),
                pltpu.make_async_copy(new, place, st.at[p, 2]),
            ]
            self.own = remote(new, place, o_s.at[c], o_r.at[c], partner)
            self.gather = self.forward = None
            if self.i < GATHERED:
                far = wi.at[l, xo, k, r]
                self.gather = remote(new, late if c == LATE else place, ax_s.at[c], ax_r.at[c], across)
                if c != LATE:
                    self.forward = remote(far, far, f_s.at[c], f_r.at[c], partner)
            else:
                for q, (layer, top, size) in enumerate(PIECES):
                    low, high = max(top, sub * rows), min(top + size, (sub + 1) * rows)
                    if layer == l and low < high:
                        part = new.at[pl.ds(low - sub * rows, high - low)]
                        self.stores.append(pltpu.make_async_copy(part, pieces[q].at[pl.ds(low - top, high - low)], st.at[p, len(self.stores)]))

    chunks = [Chunk(c) for c in range(CHUNKS)]
    chunks[0].load_b.start()

    barrier = pltpu.get_barrier_semaphore()
    for d in (partner, across):
        pl.semaphore_signal(barrier, inc=1, device_id=d, device_id_type=pl.DeviceIdType.MESH)
    pl.semaphore_wait(barrier, 2)

    def send(ch):
        for _, _, pair, _ in ch.parts:
            pair.start()

    for ch in chunks[:AHEAD]:
        send(ch)
    chunks[1].load_b.start()
    for ch in chunks:
        ch.load_b.wait()
        for at, size, pair, cross in ch.parts:
            pair.wait_recv()
            add_into(ch.rv, (ch.slot, xo), ch.ob, at, size, ch.cols)
            cross.start()
        if ch.c + AHEAD < CHUNKS:
            send(chunks[ch.c + AHEAD])
        ch.pair.start()
        if ch.c + 2 < CHUNKS:
            chunks[ch.c + 2].load_b.start()
    for ch in chunks[:2]:
        for one in ch.loads:
            one.start()
    for ch in chunks:
        for one in ch.loads:
            one.wait()
        ch.pair.wait_recv()
        for _, _, _, cross in ch.parts:
            cross.wait_recv()
        step_into(ch.xr, (ch.slot,), ch.oc, ch.rv, (ch.slot, x), ch.wc, ch.mc, ch.vc, ch.rows, ch.cols)
        if ch.gather:
            ch.gather.start()
        ch.own.start()
        for one in ch.stores:
            one.start()
        if ch.c >= 1:
            for one in chunks[ch.c - 1].stores:
                one.wait()
        if ch.c + 2 < CHUNKS:
            for one in chunks[ch.c + 2].loads:
                one.start()
    for one in chunks[-1].stores:
        one.wait()
    for ch in chunks:
        for _, _, pair, cross in ch.parts:
            pair.wait_send()
            cross.wait_send()
        ch.pair.wait_send()
        ch.own.wait()
    for ch in chunks:
        if ch.forward:
            ch.gather.wait_recv()
            ch.forward.start()
    for ch in chunks:
        if ch.forward:
            ch.gather.wait_send()
            ch.forward.wait()
    chunks[LATE].gather.wait()


def communicate(g, w, m, v):
    dims = [one.shape[3:] for one in g]
    (ra, ca), (rb, cb) = dims[0], dims[2]
    ra, rb = ra // SUBS, rb // SUBS
    sd = jax.ShapeDtypeStruct
    bf, f32 = jnp.bfloat16, jnp.float32
    dma = pltpu.SemaphoreType.DMA
    out = (
        *(sd(one.shape, bf) for one in w),
        *(sd(one.shape, f32) for one in m),
        *(sd(one.shape, f32) for one in v),
        *(sd((size, cb), bf) for _, _, size in PIECES),
        sd((ra, ca), bf),
    )
    scratch = [
        pltpu.VMEM((2 * PER, 2, ra, ca), bf), pltpu.VMEM((PER, 2, rb, cb), bf),
        pltpu.VMEM((2 * PER, ra, ca), bf), pltpu.VMEM((PER, rb, cb), bf),
        pltpu.VMEM((2, ra, ca), bf), pltpu.VMEM((2, rb, cb), bf),
        pltpu.VMEM((SLOTS, ra, ca), bf), pltpu.VMEM((SLOTS, rb, cb), bf),
        pltpu.VMEM((SLOTS, ra, ca), bf), pltpu.VMEM((SLOTS, rb, cb), bf),
        pltpu.VMEM((SLOTS, ra, ca), f32), pltpu.VMEM((SLOTS, rb, cb), f32),
        pltpu.VMEM((SLOTS, ra, ca), f32), pltpu.VMEM((SLOTS, rb, cb), f32),
        *(dma((CHUNKS + PARTS - 1,)) for _ in range(4)),
        *(dma((CHUNKS,)) for _ in range(2)),
        *(dma((GATHERED * PER,)) for _ in range(2)),
        *(dma((CHUNKS,)) for _ in range(2)),
        *(dma((LATE,)) for _ in range(2)),
        dma((2,)), dma((SLOTS, 4)), dma((SLOTS, 5)),
    ]
    return pl.pallas_call(
        functools.partial(main_kernel, dims),
        out_shape=out,
        in_specs=[ANY] * 12,
        out_specs=[ANY] * len(out),
        scratch_shapes=scratch,
        compiler_params=pltpu.CompilerParams(collective_id=0, has_side_effects=True, vmem_limit_bytes=VMEM_LIMIT),
        name="communicate",
    )(*g, *w, *m, *v)


def copy_kernel(n, _, *refs):
    for src, dst in zip(refs[:n], refs[n:], strict=True):
        dst[...] = src[...]


def copy_out(x, wf, mo, vo):
    specs = []
    for one in wf[:2]:
        rows, cols = one.shape[3:]
        specs.append(pl.BlockSpec((1, 1, 1, rows, cols), lambda i, _: (i // 4, i // 2 % 2, i % 2, 0, 0)))
    rows, cols = wf[2].shape[3:]
    specs.append(pl.BlockSpec((1, 1, 1, rows // 2, cols), lambda i, s: (i // 4, s[0], i // 2 % 2, i % 2, 0)))
    for one in (*mo, *vo):
        _, rows, cols = one.shape
        specs.append(pl.BlockSpec((1, rows // SUBS, cols), lambda i, _: (i // SUBS, i % SUBS, 0)))
    arrays = (*wf, *mo, *vo)
    size = sum(2 * one.size * one.dtype.itemsize for one in arrays)
    return pl.pallas_call(
        functools.partial(copy_kernel, len(arrays)),
        out_shape=[jax.ShapeDtypeStruct(one.shape, one.dtype) for one in arrays],
        grid_spec=pltpu.PrefetchScalarGridSpec(num_scalar_prefetch=1, grid=(PER,), in_specs=specs, out_specs=specs),
        cost_estimate=pl.CostEstimate(flops=0, bytes_accessed=size, transcendentals=0),
        compiler_params=pltpu.CompilerParams(vmem_limit_bytes=VMEM_ALL),
        name="copy_out",
    )(x.reshape(1), *arrays)


def place_kernel(l, first, near, far, whole, out, buf, ld, st):
    me = lax.axis_index("dp")
    x, k = me // 2, me % 2
    r = pl.ds(first, near.shape[0])
    loads = [pltpu.make_async_copy(near, buf.at[0], ld.at[0]), pltpu.make_async_copy(far, buf.at[1], ld.at[1])]
    stores = [
        pltpu.make_async_copy(buf.at[0], out.at[l, 1 - x, k, r], st.at[0]),
        pltpu.make_async_copy(buf.at[1], out.at[l, 1 - x, 1 - k, r], st.at[1]),
    ]
    for one in loads:
        one.start()
    for a, b in zip(loads, stores, strict=True):
        a.wait()
        b.start()
    for one in stores:
        one.wait()


def place(l, first, near, far, whole):
    return pl.pallas_call(
        functools.partial(place_kernel, l, first),
        out_shape=jax.ShapeDtypeStruct(whole.shape, whole.dtype),
        in_specs=[ANY] * 3,
        out_specs=ANY,
        scratch_shapes=[pltpu.VMEM((2, *near.shape), whole.dtype), pltpu.SemaphoreType.DMA((2,)), pltpu.SemaphoreType.DMA((2,))],
        input_output_aliases={2: 0},
        cost_estimate=pl.CostEstimate(flops=0, bytes_accessed=8 * near.size, transcendentals=0),
        compiler_params=pltpu.CompilerParams(vmem_limit_bytes=VMEM_ALL),
        name="place",
    )(near, far, whole)


def solution(mesh):
    swap_x, swap_core = [(i, (i + 2) % 4) for i in range(4)], [(i, i ^ 1) for i in range(4)]

    def step(*arrays):
        terms, weights, m, v = (arrays[i : i + 3] for i in (0, 3, 6, 9))

        def cut(a):
            return a.reshape(LAYERS, 2, 2, a.shape[-2] // 4, a.shape[-1])

        done = communicate([cut(t) for t in terms], [cut(w) for w in weights], m, v)
        wf, mo, vo, pieces, late = done[:3], done[3:6], done[6:9], done[9:-1], done[-1]
        cross = []
        for p in pieces:
            cross.append(lax.ppermute(p, "dp", swap_x))
        late_far = lax.ppermute(late, "dp", swap_core)
        x = (lax.axis_index("dp") // 2).astype(jnp.int32)
        gate, up, down, *moments = copy_out(x, wf, mo, vo)
        up = place(LAYERS - 1, (SUBS - 1) * late.shape[0], late, late_far, up)
        up, down = lax.optimization_barrier((up, down))
        for i, p in enumerate(cross):
            p, down = lax.optimization_barrier((p, down))
            far = lax.ppermute(p, "dp", swap_core)
            down = place(*PIECES[i][:2], p, far, down)
        whole = [a.reshape(w.shape) for a, w in zip((gate, up, down), weights, strict=True)]
        return (*whole, *moments)

    all_of, cut = P(None, None, None), P(None, "dp", None)
    return jax.shard_map(
        step,
        mesh=mesh,
        in_specs=(P(("rep", "dp"), None, None, None),) * 3 + (all_of,) * 3 + (cut,) * 6,
        out_specs=(P("rep", None, None),) * 3 + (P("rep", "dp", None),) * 6,
        check_vma=False,
    )
```

```python
import functools

import jax
import jax.numpy as jnp
from jax import lax
from jax.experimental import pallas as pl
from jax.experimental.pallas import tpu as pltpu
from jax.sharding import PartitionSpec as P


LAYERS = 2
SUBS = 4
PER = LAYERS * SUBS
WEIGHTS = 3
GATHERED = 2
CHUNKS = PER * WEIGHTS
SLOTS = 3
AHEAD = 4
PARTS = 4
PIECES = ((0, 0, 704), (1, 0, 480), (1, 480, 144), (1, 624, 80))
LATE = GATHERED * PER - 1
ANY = pl.BlockSpec(memory_space=pl.ANY)
VMEM_LIMIT = 60 * 2**20
WIDTH = 256


def add_into(dst, at, own, first, rows, cols):
    def body(i, _):
        r = pl.ds(pl.multiple_of(first + i * 16, 16), 16)
        for c in range(0, cols, WIDTH):
            s = pl.ds(c, WIDTH)
            dst[(*at, r, s)] = (dst[(*at, r, s)].astype(jnp.float32) + own[r, s].astype(jnp.float32)).astype(jnp.bfloat16)
        return 0

    lax.fori_loop(0, rows // 16, body, 0)


def step_into(x, at, mine, pair, pair_at, w, m, v, rows, cols):
    def body(i, _):
        r = pl.ds(pl.multiple_of(i * 16, 16), 16)
        for c in range(0, cols, WIDTH):
            s = pl.ds(c, WIDTH)
            g = mine[r, s].astype(jnp.float32) + pair[(*pair_at, r, s)].astype(jnp.float32) + x[(*at, r, s)].astype(jnp.float32)
            g = g.astype(jnp.bfloat16).astype(jnp.float32)
            nm = 0.9 * m[r, s] + 0.1 * g
            nv = 0.95 * v[r, s] + 0.05 * g * g
            old = w[r, s].astype(jnp.float32)
            step = nm * lax.rsqrt(nv + 1e-8) + 0.1 * old
            x[(*at, r, s)] = (old - 0.02 * step).astype(jnp.bfloat16)
            m[r, s] = nm
            v[r, s] = nv
        return 0

    lax.fori_loop(0, rows // 16, body, 0)


def main_kernel(dims, *refs):
    g, w, m, v = (refs[i : i + 3] for i in (0, 3, 6, 9))
    wf, mo, vo = (refs[12 + i : 15 + i] for i in (0, 3, 6))
    pieces, late = refs[21 : 21 + len(PIECES)], refs[21 + len(PIECES)]
    (rv_a, rv_b, xr_a, xr_b, ob_a, ob_b, oc_a, oc_b, wc_a, wc_b, mc_a, mc_b, vc_a, vc_b,
     e_s, e_r, x_s, x_r, d_s, d_r, ax_s, ax_r, o_s, o_r, f_s, f_r, lb, lc, st) = refs[22 + len(PIECES) :]
    me = lax.axis_index("dp")
    x, k = me // 2, me % 2
    xo, ko = 1 - x, 1 - k
    partner, across = {"dp": 2 * x + ko}, {"dp": 2 * xo + k}

    def remote(src, dst, s, r, to):
        return pltpu.make_async_remote_copy(src_ref=src, dst_ref=dst, send_sem=s, recv_sem=r, device_id=to, device_id_type=pl.DeviceIdType.MESH)

    class Chunk:
        def __init__(self, c):
            self.c, self.i = c, c // PER
            j = c % PER
            l, sub = j // SUBS, j % SUBS
            a = self.i < 2
            self.slot = slot = c if a else j
            self.rows, self.cols = rows, _ = dims[self.i][0] // SUBS, dims[self.i][1]
            r = pl.ds(sub * rows, rows)
            self.rv, self.xr = (rv_a, xr_a) if a else (rv_b, xr_b)
            self.ob = (ob_a if a else ob_b).at[c % 2]
            p = c % SLOTS
            self.oc, self.wc, self.mc, self.vc = (t.at[p] for t in ((oc_a, wc_a, mc_a, vc_a) if a else (oc_b, wc_b, mc_b, vc_b)))
            gi, wi = g[self.i], wf[self.i]
            n = PARTS if c == 0 else 1
            self.parts = []
            for q in range(n):
                at, size, sem = q * rows // n, rows // n, q if c == 0 else c + PARTS - 1
                src = gi.at[l, xo, ko, pl.ds(sub * rows + at, size)]
                sums = self.rv.at[slot, xo, pl.ds(at, size)]
                sums_there = self.rv.at[slot, xo, pl.ds(at, size)]
                pair = remote(src, sums_there, e_s.at[sem], e_r.at[sem], partner)
                cross = remote(sums, self.xr.at[slot, pl.ds(at, size)], x_s.at[sem], x_r.at[sem], across)
                self.parts.append((at, size, pair, cross))
            self.pair = remote(gi.at[l, x, ko, r], self.rv.at[slot, x], d_s.at[c], d_r.at[c], partner)
            self.load_b = pltpu.make_async_copy(gi.at[l, xo, k, r], self.ob, lb.at[c % 2])
            block = (l, r)
            self.loads = [
                pltpu.make_async_copy(gi.at[l, x, k, r], self.oc, lc.at[p, 0]),
                pltpu.make_async_copy(w[self.i].at[l, x, k, r], self.wc, lc.at[p, 1]),
                pltpu.make_async_copy(m[self.i].at[block], self.mc, lc.at[p, 2]),
                pltpu.make_async_copy(v[self.i].at[block], self.vc, lc.at[p, 3]),
            ]
            new, place = self.xr.at[slot], wi.at[l, x, k, r]
            self.stores = [
                pltpu.make_async_copy(self.mc, mo[self.i].at[block], st.at[p, 0]),
                pltpu.make_async_copy(self.vc, vo[self.i].at[block], st.at[p, 1]),
                pltpu.make_async_copy(new, place, st.at[p, 2]),
            ]
            self.own = remote(new, place, o_s.at[c], o_r.at[c], partner)
            self.gather = self.forward = None
            if self.i < GATHERED:
                far = wi.at[l, xo, k, r]
                self.gather = remote(new, late if c == LATE else place, ax_s.at[c], ax_r.at[c], across)
                if c != LATE:
                    self.forward = remote(far, far, f_s.at[c], f_r.at[c], partner)
            else:
                for q, (layer, top, size) in enumerate(PIECES):
                    low, high = max(top, sub * rows), min(top + size, (sub + 1) * rows)
                    if layer == l and low < high:
                        part = new.at[pl.ds(low - sub * rows, high - low)]
                        self.stores.append(pltpu.make_async_copy(part, pieces[q].at[pl.ds(low - top, high - low)], st.at[p, len(self.stores)]))

    chunks = [Chunk(c) for c in range(CHUNKS)]
    chunks[0].load_b.start()

    barrier = pltpu.get_barrier_semaphore()
    for d in (partner, across):
        pl.semaphore_signal(barrier, inc=1, device_id=d, device_id_type=pl.DeviceIdType.MESH)
    pl.semaphore_wait(barrier, 2)

    def send(ch):
        for _, _, pair, _ in ch.parts:
            pair.start()

    for ch in chunks[:AHEAD]:
        send(ch)
    chunks[1].load_b.start()
    for ch in chunks:
        ch.load_b.wait()
        for at, size, pair, cross in ch.parts:
            pair.wait_recv()
            add_into(ch.rv, (ch.slot, xo), ch.ob, at, size, ch.cols)
            cross.start()
        if ch.c + AHEAD < CHUNKS:
            send(chunks[ch.c + AHEAD])
        ch.pair.start()
        if ch.c + 2 < CHUNKS:
            chunks[ch.c + 2].load_b.start()
    for ch in chunks[:2]:
        for one in ch.loads:
            one.start()
    for ch in chunks:
        for one in ch.loads:
            one.wait()
        ch.pair.wait_recv()
        for _, _, _, cross in ch.parts:
            cross.wait_recv()
        step_into(ch.xr, (ch.slot,), ch.oc, ch.rv, (ch.slot, x), ch.wc, ch.mc, ch.vc, ch.rows, ch.cols)
        if ch.gather:
            ch.gather.start()
        ch.own.start()
        for one in ch.stores:
            one.start()
        if ch.c >= 1:
            for one in chunks[ch.c - 1].stores:
                one.wait()
        if ch.c + 2 < CHUNKS:
            for one in chunks[ch.c + 2].loads:
                one.start()
    for one in chunks[-1].stores:
        one.wait()
    for ch in chunks:
        for _, _, pair, cross in ch.parts:
            pair.wait_send()
            cross.wait_send()
        ch.pair.wait_send()
        ch.own.wait()
    for ch in chunks:
        if ch.forward:
            ch.gather.wait_recv()
            ch.forward.start()
    for ch in chunks:
        if ch.forward:
            ch.gather.wait_send()
            ch.forward.wait()
    chunks[LATE].gather.wait()


def communicate(g, w, m, v):
    dims = [one.shape[3:] for one in g]
    (ra, ca), (rb, cb) = dims[0], dims[2]
    ra, rb = ra // SUBS, rb // SUBS
    sd = jax.ShapeDtypeStruct
    bf, f32 = jnp.bfloat16, jnp.float32
    dma = pltpu.SemaphoreType.DMA
    out = (
        *(sd(one.shape, bf) for one in w),
        *(sd(one.shape, f32) for one in m),
        *(sd(one.shape, f32) for one in v),
        *(sd((size, cb), bf) for _, _, size in PIECES),
        sd((ra, ca), bf),
    )
    scratch = [
        pltpu.VMEM((2 * PER, 2, ra, ca), bf), pltpu.VMEM((PER, 2, rb, cb), bf),
        pltpu.VMEM((2 * PER, ra, ca), bf), pltpu.VMEM((PER, rb, cb), bf),
        pltpu.VMEM((2, ra, ca), bf), pltpu.VMEM((2, rb, cb), bf),
        pltpu.VMEM((SLOTS, ra, ca), bf), pltpu.VMEM((SLOTS, rb, cb), bf),
        pltpu.VMEM((SLOTS, ra, ca), bf), pltpu.VMEM((SLOTS, rb, cb), bf),
        pltpu.VMEM((SLOTS, ra, ca), f32), pltpu.VMEM((SLOTS, rb, cb), f32),
        pltpu.VMEM((SLOTS, ra, ca), f32), pltpu.VMEM((SLOTS, rb, cb), f32),
        *(dma((CHUNKS + PARTS - 1,)) for _ in range(4)),
        *(dma((CHUNKS,)) for _ in range(2)),
        *(dma((GATHERED * PER,)) for _ in range(2)),
        *(dma((CHUNKS,)) for _ in range(2)),
        *(dma((LATE,)) for _ in range(2)),
        dma((2,)), dma((SLOTS, 4)), dma((SLOTS, 5)),
    ]
    return pl.pallas_call(
        functools.partial(main_kernel, dims),
        out_shape=out,
        in_specs=[ANY] * 12,
        out_specs=[ANY] * len(out),
        scratch_shapes=scratch,
        compiler_params=pltpu.CompilerParams(collective_id=0, has_side_effects=True, vmem_limit_bytes=VMEM_LIMIT),
        name="communicate",
    )(*g, *w, *m, *v)


def copy_kernel(n, _, *refs):
    for src, dst in zip(refs[:n], refs[n:], strict=True):
        dst[...] = src[...]


def copy_out(x, wf, mo, vo):
    specs = []
    for one in wf[:2]:
        rows, cols = one.shape[3:]
        specs.append(pl.BlockSpec((1, 1, 1, rows, cols), lambda i, _: (i // 4, i // 2 % 2, i % 2, 0, 0)))
    rows, cols = wf[2].shape[3:]
    specs.append(pl.BlockSpec((1, 1, 1, rows // 2, cols), lambda i, s: (i // 4, s[0], i // 2 % 2, i % 2, 0)))
    for one in (*mo, *vo):
        _, rows, cols = one.shape
        specs.append(pl.BlockSpec((1, rows // SUBS, cols), lambda i, _: (i // SUBS, i % SUBS, 0)))
    arrays = (*wf, *mo, *vo)
    size = sum(2 * one.size * one.dtype.itemsize for one in arrays)
    return pl.pallas_call(
        functools.partial(copy_kernel, len(arrays)),
        out_shape=[jax.ShapeDtypeStruct(one.shape, one.dtype) for one in arrays],
        grid_spec=pltpu.PrefetchScalarGridSpec(num_scalar_prefetch=1, grid=(PER,), in_specs=specs, out_specs=specs),
        cost_estimate=pl.CostEstimate(flops=0, bytes_accessed=size, transcendentals=0),
        compiler_params=pltpu.CompilerParams(vmem_limit_bytes=40 * 2**20),
        name="copy_out",
    )(x.reshape(1), *arrays)


def place_kernel(l, first, near, far, whole, out, st):
    me = lax.axis_index("dp")
    x, k = me // 2, me % 2
    r = pl.ds(first, near.shape[0])
    stores = [
        pltpu.make_async_copy(near, out.at[l, 1 - x, k, r], st.at[0]),
        pltpu.make_async_copy(far, out.at[l, 1 - x, 1 - k, r], st.at[1]),
    ]
    for one in stores:
        one.start()
    for one in stores:
        one.wait()


def place(l, first, near, far, whole):
    return pl.pallas_call(
        functools.partial(place_kernel, l, first),
        out_shape=jax.ShapeDtypeStruct(whole.shape, whole.dtype),
        in_specs=[pl.BlockSpec(memory_space=pltpu.VMEM)] * 2 + [ANY],
        out_specs=ANY,
        scratch_shapes=[pltpu.SemaphoreType.DMA((2,))],
        input_output_aliases={2: 0},
        cost_estimate=pl.CostEstimate(flops=0, bytes_accessed=8 * near.size, transcendentals=0),
        compiler_params=pltpu.CompilerParams(vmem_limit_bytes=2 * 2**20),
        name="place",
    )(near, far, whole)


def solution(mesh):
    swap_x, swap_core = [(i, (i + 2) % 4) for i in range(4)], [(i, i ^ 1) for i in range(4)]

    def step(*arrays):
        terms, weights, m, v = (arrays[i : i + 3] for i in (0, 3, 6, 9))

        def cut(a):
            return a.reshape(LAYERS, 2, 2, a.shape[-2] // 4, a.shape[-1])

        done = communicate([cut(t) for t in terms], [cut(w) for w in weights], m, v)
        wf, mo, vo, pieces, late = done[:3], done[3:6], done[6:9], done[9:-1], done[-1]
        cross = []
        for p in pieces:
            cross.append(lax.ppermute(p, "dp", swap_x))
        late_far = lax.ppermute(late, "dp", swap_core)
        x = (lax.axis_index("dp") // 2).astype(jnp.int32)
        gate, up, down, *moments = copy_out(x, wf, mo, vo)
        up = place(LAYERS - 1, (SUBS - 1) * late.shape[0], late, late_far, up)
        up, down = lax.optimization_barrier((up, down))
        for i, p in enumerate(cross):
            p, down = lax.optimization_barrier((p, down))
            far = lax.ppermute(p, "dp", swap_core)
            down = place(*PIECES[i][:2], p, far, down)
        whole = [a.reshape(w.shape) for a, w in zip((gate, up, down), weights, strict=True)]
        return (*whole, *moments)

    all_of, cut = P(None, None, None), P(None, "dp", None)
    return jax.shard_map(
        step,
        mesh=mesh,
        in_specs=(P(("rep", "dp"), None, None, None),) * 3 + (all_of,) * 3 + (cut,) * 6,
        out_specs=(P("rep", None, None),) * 3 + (P("rep", "dp", None),) * 6,
        check_vma=False,
    )
```
